32 devices in a mesh: cls: 4 (over y, x), row: 8 (over z, core).
Axes of the slice: x: 2, y: 2, z: 4, core: 2. Of those that a mesh axis runs over, the one named last changes fastest.
Arguments:
- binned: int32 [32768, 512], P('row'), may hold values from 0 to 255
- labels: int32 [32768], P('row'), may hold values from 0 to 127
- logits: float32 [32768, 128], P('row', 'cls'), may hold values from -320 to 320
- elected: int32 [128, 12], P('cls'), may hold values from 0 to 511, as said below
- split_slot: int32 [128], P('cls'), may hold values from 0 to 11
- split_bin: int32 [128], P('cls'), may hold values from 0 to 254
Outputs:
- new_logits: float32 [32768, 128], P('row', 'cls')
- split_gains: float32 [128, 12, 256], P(('cls', 'row'))
The draws below stay inside these ranges and needn't reach their ends.
Inputs may be any that keep to these rules, and one draw needn't show every extreme that they name: `elected`: the 12 ids of one class are distinct.
All inputs are finite; a program needn't handle non-finite values.
Results may differ from the reference program's by a relative error of at most 0.002.
Values sent between devices are 32-bit elements; how exact they have to be, the bound alone decides.
A program may use at most 128 MiB of HBM per device.

```python
import jax
import jax.numpy as jnp
from jax import lax

F = 512
B = 256
K = 12
CLASSES = 128
ROWS = 32768


def draw_logits(key, part):
    normal_key = jax.random.fold_in(key, 0)
    scores = 2.0 * jnp.clip(jax.random.normal(normal_key, (ROWS, CLASSES), jnp.float32), -6.0, 6.0)
    return scores


def draw_elected(key, part):
    class_keys = jax.random.split(key, CLASSES)

    def choose_ids(class_key):
        return jax.random.permutation(class_key, F)[:K].astype(jnp.int32)
    return jax.vmap(choose_ids)(class_keys)


def place_ends(array, key, low, high):
    dims = array.shape
    index_at = [jax.random.randint(jax.random.fold_in(key, axis), (), 0, dims[axis]) for axis in range(len(dims))]
    array = array.at[tuple(index_at)].set(low)
    longest = dims.index(max(dims))
    index_at[longest] = (index_at[longest] + 1) % dims[longest]
    return array.at[tuple(index_at)].set(high)


def setup_inputs(seed: int = 0) -> dict:
    keys = jax.random.split(jax.random.key(seed), 7)
    return {
        "binned": place_ends(jax.random.randint(keys[0], (ROWS, F), 0, B), jax.random.fold_in(keys[0], 1), 0, B - 1).astype(jnp.int32),
        "labels": place_ends(jax.random.randint(keys[1], (ROWS,), 0, CLASSES), jax.random.fold_in(keys[1], 1), 0, CLASSES - 1).astype(jnp.int32),
        "logits": draw_logits(jax.random.fold_in(keys[6], 71), 0),
        "elected": draw_elected(jax.random.fold_in(keys[6], 71), 0),
        "split_slot": place_ends(jax.random.randint(keys[4], (CLASSES,), 0, K), jax.random.fold_in(keys[4], 1), 0, K - 1).astype(jnp.int32),
        "split_bin": place_ends(jax.random.randint(keys[5], (CLASSES,), 0, B - 1), jax.random.fold_in(keys[5], 1), 0, (B - 1) - 1).astype(jnp.int32),
    }


reg_lambda = 1.0
step_rate = 0.5


def reference(binned, labels, logits, elected, split_slot, split_bin):
    highest = jnp.max(logits, axis=1, keepdims=True)
    shifted = jnp.exp(logits - highest)
    total = jnp.sum(shifted, axis=1, keepdims=True)
    probs = shifted / total
    class_ids = jnp.arange(CLASSES, dtype=jnp.int32)
    target = (labels[:, None] == class_ids[None, :]).astype(jnp.float32)
    gradient = (probs - target).astype(jnp.bfloat16)
    hessian = (probs * (1.0 - probs)).astype(jnp.bfloat16)

    def per_class(index):
        columns = jnp.take(binned, elected[index], axis=1)
        grad_col = lax.dynamic_slice_in_dim(gradient, index, 1, 1)[:, 0]
        hess_col = lax.dynamic_slice_in_dim(hessian, index, 1, 1)[:, 0]
        weights = jnp.stack([grad_col, hess_col], axis=1).astype(jnp.float32)

        def per_feature(column):
            return jax.ops.segment_sum(weights, column, num_segments=B)

        return jax.vmap(per_feature, in_axes=1)(columns)

    histogram = lax.map(per_class, class_ids)
    histogram = jnp.transpose(histogram, (0, 1, 3, 2))
    running = jnp.cumsum(histogram, axis=-1)
    grad_left = running[:, :, 0, :]
    hess_left = running[:, :, 1, :]
    grad_all = grad_left[:, :, -1:]
    hess_all = hess_left[:, :, -1:]
    split_gains = (grad_left * grad_left / (hess_left + reg_lambda)
                   + (grad_all - grad_left) ** 2 / (hess_all - hess_left + reg_lambda)
                   - grad_all * grad_all / (hess_all + reg_lambda))
    grad_row = jnp.take_along_axis(grad_left, split_slot[:, None, None], axis=1)[:, 0, :]
    hess_row = jnp.take_along_axis(hess_left, split_slot[:, None, None], axis=1)[:, 0, :]
    grad_split = jnp.take_along_axis(grad_row, split_bin[:, None], axis=1)[:, 0]
    hess_split = jnp.take_along_axis(hess_row, split_bin[:, None], axis=1)[:, 0]
    left_leaf = -grad_split / (hess_split + reg_lambda)
    right_leaf = -(grad_row[:, -1] - grad_split) / (hess_row[:, -1] - hess_split + reg_lambda)
    chosen_feature = jnp.take_along_axis(elected, split_slot[:, None], axis=1)[:, 0]
    chosen_bins = jnp.take(binned, chosen_feature, axis=1)
    goes_left = chosen_bins <= split_bin[None, :]
    new_logits = logits + step_rate * jnp.where(goes_left, left_leaf[None, :], right_leaf[None, :])
    return new_logits, split_gains
```

```python
import functools
import math

import jax
import jax.numpy as jnp
from jax import lax
from jax.experimental import pallas as pl
from jax.experimental.pallas import tpu as pltpu
from jax.sharding import PartitionSpec as P

reg_lambda = 1.0
step_rate = 0.5
MESH = pl.DeviceIdType.MESH
NT = (((1,), (1,)), ((), ()))
LOW = 32
HIGH = 8
BINS = LOW * HIGH


def stats_kernel(n_cls, x_ref, labels_ref, grad_ref, hess_ref, stats, send_sem, recv_sem):
    me = lax.axis_index("cls")
    row = lax.axis_index("row")
    barrier = pltpu.get_barrier_semaphore()
    for step in range(1, n_cls):
        peer = lax.rem(me + step, n_cls)
        pl.semaphore_signal(barrier, inc=1, device_id=(peer, row), device_id_type=MESH)
    x = x_ref[...]
    classes = x.shape[0]
    local_max = jnp.max(x, axis=0, keepdims=True)
    local_sum = jnp.sum(jnp.exp(x - local_max), axis=0, keepdims=True)
    stats[0, 0:1, :] = local_max
    stats[0, 1:2, :] = local_sum
    pl.semaphore_wait(barrier, n_cls - 1)
    copies = []
    for step in range(1, n_cls):
        peer = lax.rem(me + step, n_cls)
        copy = pltpu.make_async_remote_copy(
            src_ref=stats.at[0],
            dst_ref=stats.at[step],
            send_sem=send_sem.at[step],
            recv_sem=recv_sem.at[step],
            device_id=(peer, row),
            device_id_type=MESH,
        )
        copy.start()
        copies.append(copy)
    for copy in copies:
        copy.wait()
    highest = local_max
    for step in range(1, n_cls):
        highest = jnp.maximum(highest, stats[step, 0:1, :])
    total = local_sum * jnp.exp(local_max - highest)
    for step in range(1, n_cls):
        total = total + stats[step, 1:2, :] * jnp.exp(stats[step, 0:1, :] - highest)
    probs = jnp.exp(x_ref[...] - highest) / total
    class_ids = me * classes + lax.broadcasted_iota(jnp.int32, x.shape, 0)
    target = (labels_ref[...] == class_ids).astype(jnp.float32)
    grad_ref[...] = (probs - target).astype(jnp.bfloat16).astype(jnp.float32)
    hess_ref[...] = (probs * (1.0 - probs)).astype(jnp.bfloat16).astype(jnp.float32)


def histogram_kernel(
    group, chunk, features, binned_ref, ids_ref, split_ref, grad_ref, hess_ref,
    hist_ref, left_ref, sums_ref, picker, low, high, weights,
):
    step = pl.program_id(0)
    block = binned_ref.shape[0]
    classes, rows = grad_ref.shape
    pairs = low.shape[0]

    @pl.when(step == 0)
    def _():
        picker[...] = (
            lax.broadcasted_iota(jnp.int32, picker.shape, 1) == ids_ref[...]
        ).astype(jnp.float32).astype(jnp.bfloat16)

    here = binned_ref[...].astype(jnp.float32).astype(jnp.bfloat16)
    picked = lax.dot_general(picker[...], here, NT, preferred_element_type=jnp.float32)
    picked = picked.astype(jnp.int32)
    where = pl.ds(pl.multiple_of(step * block, block), block)
    chosen = picked[:pairs]
    low[:, where] = (chosen & (LOW - 1)).astype(jnp.float32)
    high[:, where] = (chosen >> 5).astype(jnp.float32)
    left_ref[:, where] = (picked[pairs:] <= split_ref[...]).astype(jnp.float32)

    @pl.when(step == pl.num_programs(0) - 1)
    def _():
        grad = grad_ref[...]
        hess = hess_ref[...]
        left = left_ref[...]
        lane = lax.broadcasted_iota(jnp.int32, sums_ref.shape, 1)
        total = jnp.where(lane == 0, jnp.sum(grad * left, axis=1, keepdims=True), 0.0)
        total = jnp.where(lane == 1, jnp.sum(hess * left, axis=1, keepdims=True), total)
        total = jnp.where(lane == 2, jnp.sum(grad, axis=1, keepdims=True), total)
        total = jnp.where(lane == 3, jnp.sum(hess, axis=1, keepdims=True), total)
        sums_ref[...] = total

        is_grad = lax.broadcasted_iota(jnp.int32, (2 * HIGH, rows), 0) < HIGH

        def expand(c, carry):
            mixed = jnp.where(is_grad, grad_ref[pl.ds(c, 1), :], hess_ref[pl.ds(c, 1), :])
            weights[pl.ds(pl.multiple_of(c * 2 * HIGH, 2 * HIGH), 2 * HIGH), :] = mixed.astype(
                jnp.bfloat16
            )
            return carry

        lax.fori_loop(0, classes, expand, 0)

        sub = lax.broadcasted_iota(jnp.int32, (16, chunk), 0)
        low_first = sub.astype(jnp.float32).astype(jnp.bfloat16)
        low_second = (sub + 16).astype(jnp.float32).astype(jnp.bfloat16)
        high_ids = (sub & (HIGH - 1)).astype(jnp.float32).astype(jnp.bfloat16)
        one = jnp.ones((16, chunk), jnp.bfloat16)
        zero = jnp.zeros((16, chunk), jnp.bfloat16)
        lane_pair = lax.broadcasted_iota(jnp.int32, (2 * HIGH, group * LOW), 1) // LOW

        def one_group(g, carry):
            total = None
            for part in range(rows // chunk):
                cols = pl.ds(part * chunk, chunk)
                lows = []
                highs = []
                for j in range(group):
                    p = g * group + j
                    c = p // features
                    lo = jnp.broadcast_to(low[pl.ds(p, 1), cols], (16, chunk)).astype(jnp.bfloat16)
                    hi = jnp.broadcast_to(high[pl.ds(p, 1), cols], (16, chunk)).astype(jnp.bfloat16)
                    w = weights[pl.ds(pl.multiple_of(c * 16, 16), 16), cols]
                    lows.append(jnp.where(lo == low_first, one, zero))
                    lows.append(jnp.where(lo == low_second, one, zero))
                    highs.append(jnp.where(hi == high_ids, w, zero))
                product = lax.dot_general(
                    jnp.concatenate(highs, axis=0), jnp.concatenate(lows, axis=0), NT,
                    preferred_element_type=jnp.float32,
                )
                total = product if total is None else total + product
            kept = total[:16]
            for j in range(1, group):
                kept = jnp.where(lane_pair == j, total[16 * j : 16 * j + 16], kept)
            hist_ref[g] = kept
            return carry

        lax.fori_loop(0, pairs // group, one_group, 0)


def finish_kernel(
    n_row, groups_each, group, hist_ref, x_ref, left_ref, sums_ref, new_ref, gains_ref,
    first, second, mine, all_sums, send_one, recv_one, send_two, recv_two, send_sum, recv_sum,
):
    cls = lax.axis_index("cls")
    me = lax.axis_index("row")
    core = lax.rem(me, 2)
    chip = me // 2
    chips = n_row // 2
    barrier = pltpu.get_barrier_semaphore()
    for step in range(1, n_row):
        peer = lax.rem(me + step, n_row)
        pl.semaphore_signal(barrier, inc=1, device_id=(cls, peer), device_id_type=MESH)
    pl.semaphore_wait(barrier, n_row - 1)

    def block_of(dest):
        return hist_ref.at[pl.ds(dest * groups_each, groups_each)]

    ones = []
    order = [lax.rem(chip + step, chips) for step in list(range(1, chips)) + [0]]
    for step in range(chips):
        copy = pltpu.make_async_remote_copy(
            src_ref=block_of(2 * order[step] + 1 - core),
            dst_ref=first.at[step],
            send_sem=send_one.at[step],
            recv_sem=recv_one.at[step],
            device_id=(cls, 2 * chip + 1 - core),
            device_id_type=MESH,
        )
        copy.start()
        ones.append(copy)
    sums = []
    for step in range(1, n_row):
        peer = lax.rem(me + step, n_row)
        copy = pltpu.make_async_remote_copy(
            src_ref=sums_ref,
            dst_ref=all_sums.at[step],
            send_sem=send_sum.at[step],
            recv_sem=recv_sum.at[step],
            device_id=(cls, peer),
            device_id_type=MESH,
        )
        copy.start()
        sums.append(copy)
    twos = []
    for step in range(chips):
        ones[step].wait_recv()
        mine[step] = first[step] + hist_ref[pl.ds((2 * order[step] + core) * groups_each, groups_each)]
        if step < chips - 1:
            copy = pltpu.make_async_remote_copy(
                src_ref=mine.at[step],
                dst_ref=second.at[step],
                send_sem=send_two.at[step],
                recv_sem=recv_two.at[step],
                device_id=(cls, 2 * order[step] + core),
                device_id_type=MESH,
            )
            copy.start()
            twos.append(copy)
    total = sums_ref[...]
    for step in range(1, n_row):
        sums[step - 1].wait()
        total = total + all_sums[step]
    grad_left = total[:, 0:1]
    hess_left = total[:, 1:2]
    left_leaf = -grad_left / (hess_left + reg_lambda)
    right_leaf = -(total[:, 2:3] - grad_left) / (total[:, 3:4] - hess_left + reg_lambda)
    new_ref[...] = x_ref[...] + step_rate * jnp.where(left_ref[...] > 0.5, left_leaf, right_leaf)

    summed = mine[chips - 1]
    for copy in ones:
        copy.wait_send()
    for step in range(chips - 1):
        twos[step].wait()
        summed = summed + second[step]
    wide = group * LOW
    here = summed.reshape(groups_each * 2 * HIGH, wide)
    a = lax.broadcasted_iota(jnp.int32, (wide, wide), 0)
    b = lax.broadcasted_iota(jnp.int32, (wide, wide), 1)
    same = (a // LOW) == (b // LOW)
    upto = (same & (a <= b)).astype(jnp.float32)
    every = same.astype(jnp.float32)
    inside = jnp.dot(here, upto, precision=lax.Precision.HIGHEST, preferred_element_type=jnp.float32)
    whole = jnp.dot(here, every, precision=lax.Precision.HIGHEST, preferred_element_type=jnp.float32)
    count = groups_each * 2 * HIGH
    r = lax.broadcasted_iota(jnp.int32, (count, count), 0)
    s = lax.broadcasted_iota(jnp.int32, (count, count), 1)
    same_high = (r // HIGH) == (s // HIGH)
    before = jnp.dot((same_high & (s < r)).astype(jnp.float32), whole,
                     precision=lax.Precision.HIGHEST, preferred_element_type=jnp.float32)
    ends = jnp.dot(same_high.astype(jnp.float32), whole,
                   precision=lax.Precision.HIGHEST, preferred_element_type=jnp.float32)
    running = inside + before
    for g in range(groups_each):
        top = g * 2 * HIGH
        gl = running[top : top + HIGH]
        hl = running[top + HIGH : top + 2 * HIGH]
        ga = ends[top : top + HIGH]
        ha = ends[top + HIGH : top + 2 * HIGH]
        gains_ref[g] = (
            gl * gl / (hl + reg_lambda)
            + (ga - gl) * (ga - gl) / (ha - hl + reg_lambda)
            - ga * ga / (ha + reg_lambda)
        )


VMEM = pl.BlockSpec(memory_space=pltpu.VMEM)


def local(n_cls, n_row, binned, labels, logits, elected, split_slot, split_bin):
    rows, classes = logits.shape
    columns = binned.shape[1]
    features = elected.shape[1]
    pairs = classes * features
    share = classes // n_row
    group = math.gcd(share * features, 8)
    groups = pairs // group
    groups_each = groups // n_row
    block = math.gcd(rows, 512)
    chunk = math.gcd(rows, 1024)
    f32 = jnp.float32
    x = logits.T
    dma = pltpu.SemaphoreType.DMA

    grad, hess = pl.pallas_call(
        functools.partial(stats_kernel, n_cls),
        out_shape=[jax.ShapeDtypeStruct((classes, rows), f32)] * 2,
        in_specs=[VMEM] * 2,
        out_specs=[VMEM] * 2,
        scratch_shapes=[pltpu.VMEM((n_cls, 2, rows), f32), dma((n_cls,)), dma((n_cls,))],
        compiler_params=pltpu.CompilerParams(collective_id=0, has_side_effects=True),
        name="stats",
    )(x, labels.reshape(1, rows))

    slot_mask = jnp.arange(features, dtype=jnp.int32)[None, :] == split_slot[:, None]
    split_feature = jnp.sum(jnp.where(slot_mask, elected, 0), axis=1)
    ids = jnp.concatenate([elected.reshape(-1), split_feature]).reshape(pairs + classes, 1)

    def whole(*shape):
        return pl.BlockSpec(shape, lambda i: (0,) * len(shape))

    hist, left, sums = pl.pallas_call(
        functools.partial(histogram_kernel, group, chunk, features),
        grid=(rows // block,),
        out_shape=[
            jax.ShapeDtypeStruct((groups, 2 * HIGH, group * LOW), f32),
            jax.ShapeDtypeStruct((classes, rows), f32),
            jax.ShapeDtypeStruct((classes, 128), f32),
        ],
        in_specs=[
            pl.BlockSpec((block, columns), lambda i: (i, 0)),
            whole(pairs + classes, 1),
            whole(classes, 1),
            whole(classes, rows),
            whole(classes, rows),
        ],
        out_specs=[whole(groups, 2 * HIGH, group * LOW), whole(classes, rows), whole(classes, 128)],
        scratch_shapes=[
            pltpu.VMEM((pairs + classes, columns), jnp.bfloat16),
            pltpu.VMEM((pairs, rows), f32),
            pltpu.VMEM((pairs, rows), f32),
            pltpu.VMEM((classes * 2 * HIGH, rows), jnp.bfloat16),
        ],
        compiler_params=pltpu.CompilerParams(
            dimension_semantics=("arbitrary",), vmem_limit_bytes=56 * 1024 * 1024
        ),
        name="histogram",
    )(binned, ids, split_bin.reshape(classes, 1), grad, hess)

    chips = n_row // 2
    part = (groups_each, 2 * HIGH, group * LOW)
    new, gains = pl.pallas_call(
        functools.partial(finish_kernel, n_row, groups_each, group),
        out_shape=[
            jax.ShapeDtypeStruct((classes, rows), f32),
            jax.ShapeDtypeStruct((groups_each, HIGH, group * LOW), f32),
        ],
        in_specs=[VMEM] * 4,
        out_specs=[VMEM] * 2,
        scratch_shapes=[
            pltpu.VMEM((chips,) + part, f32),
            pltpu.VMEM((chips,) + part, f32),
            pltpu.VMEM((chips,) + part, f32),
            pltpu.VMEM((n_row, classes, 128), f32),
            dma((chips,)), dma((chips,)), dma((chips,)), dma((chips,)),
            dma((n_row,)), dma((n_row,)),
        ],
        compiler_params=pltpu.CompilerParams(collective_id=1, has_side_effects=True),
        name="finish",
    )(hist, x, left, sums)
    gains = gains.reshape(groups_each, HIGH, group, LOW).transpose(0, 2, 1, 3)
    return new.T, gains.reshape(share, features, BINS)


def solution(mesh):
    return jax.shard_map(
        functools.partial(local, mesh.shape["cls"], mesh.shape["row"]),
        mesh=mesh,
        in_specs=(P("row", None), P("row"), P("row", "cls"), P("cls", None), P("cls"), P("cls")),
        out_specs=(P("row", "cls"), P(("cls", "row"), None, None)),
        check_vma=False,
    )
```

```python
import functools
import math

import jax
import jax.numpy as jnp
from jax import lax
from jax.experimental import pallas as pl
from jax.experimental.pallas import tpu as pltpu
from jax.experimental.layout import Layout, with_layout_constraint
from jax.sharding import PartitionSpec as P

reg_lambda = 1.0
step_rate = 0.5
MESH = pl.DeviceIdType.MESH
NT = (((1,), (1,)), ((), ()))
LOW = 32
HIGH = 8
BINS = LOW * HIGH
UNROLL = 2
CHUNK = 1024
BLOCK = 512


def kernel(
    n_cls, n_row, group, groups_each, chunk, unroll,
    binned_ref, x_ref, labels_ref, elected_ref, slot_ref, split_ref,
    new_ref, gains_ref,
    meta, picker, low, high, left, weights, grad_ref, hess_ref, stats, sums,
    theirs, mine, first, second,
    send_stat, recv_stat, send_sum, recv_sum, send_one, recv_one, send_two, recv_two,
):
    step = pl.program_id(0)
    last = pl.num_programs(0) - 1
    block = binned_ref.shape[0]
    classes, rows = x_ref.shape
    features = elected_ref.shape[0]
    pairs = classes * features
    cls = lax.axis_index("cls")
    me = lax.axis_index("row")
    core = lax.rem(me, 2)
    chip = me // 2
    chips = n_row // 2
    barrier = pltpu.get_barrier_semaphore()

    def stat_copy(k):
        return pltpu.make_async_remote_copy(
            src_ref=stats.at[0], dst_ref=stats.at[k], send_sem=send_stat.at[k], recv_sem=recv_stat.at[k],
            device_id=(lax.rem(cls + k, n_cls), me), device_id_type=MESH,
        )

    def sum_copy(k):
        return pltpu.make_async_remote_copy(
            src_ref=sums.at[0], dst_ref=sums.at[k], send_sem=send_sum.at[k], recv_sem=recv_sum.at[k],
            device_id=(cls, lax.rem(me + k, n_row)), device_id_type=MESH,
        )

    def one_copy(s):
        return pltpu.make_async_remote_copy(
            src_ref=theirs.at[s], dst_ref=first.at[s], send_sem=send_one.at[s], recv_sem=recv_one.at[s],
            device_id=(cls, 2 * chip + 1 - core), device_id_type=MESH,
        )

    def two_copy(s):
        return pltpu.make_async_remote_copy(
            src_ref=mine.at[s], dst_ref=second.at[s], send_sem=send_two.at[s], recv_sem=recv_two.at[s],
            device_id=(cls, 2 * lax.rem(chip + s + 1, chips) + core), device_id_type=MESH,
        )

    @pl.when(step == 0)
    def _():
        for k in range(1, n_cls):
            pl.semaphore_signal(
                barrier, inc=1, device_id=(lax.rem(cls + k, n_cls), me), device_id_type=MESH
            )
        for k in range(1, n_row):
            pl.semaphore_signal(
                barrier, inc=1, device_id=(cls, lax.rem(me + k, n_row)), device_id_type=MESH
            )
        x = x_ref[...]
        local_max = jnp.max(x, axis=0, keepdims=True)
        stats[0, 0:1, :] = local_max
        stats[0, 1:2, :] = jnp.sum(jnp.exp(x - local_max), axis=0, keepdims=True)
        meta[...] = jnp.zeros(meta.shape, jnp.float32)
        meta[:features, :classes] = elected_ref[...].astype(jnp.float32)
        meta[features : features + 1, :classes] = slot_ref[...].astype(jnp.float32)
        meta[features + 1 : features + 2, :classes] = split_ref[...].astype(jnp.float32)
        turned = meta[...].T
        meta[...] = turned
        lane = lax.broadcasted_iota(jnp.int32, (classes, picker.shape[1]), 1).astype(jnp.float32)
        slot = turned[:classes, features : features + 1]
        split_feature = jnp.zeros((classes, 1), jnp.float32)
        for k in range(features):
            column = turned[:classes, k : k + 1]
            split_feature = jnp.where(slot == k, column, split_feature)
            picker[k * classes : (k + 1) * classes] = (lane == column).astype(jnp.float32).astype(
                jnp.bfloat16
            )
        picker[pairs:] = (lane == split_feature).astype(jnp.float32).astype(jnp.bfloat16)
        pl.semaphore_wait(barrier, n_cls - 1 + n_row - 1)
        for k in range(1, n_cls):
            stat_copy(k).start()

    here = binned_ref[...].astype(jnp.float32).astype(jnp.bfloat16)
    picked = lax.dot_general(picker[...], here, NT, preferred_element_type=jnp.float32)
    where = pl.ds(pl.multiple_of(step * block, block), block)
    chosen = picked[:pairs].astype(jnp.int32)
    low[:, where] = (chosen & (LOW - 1)).astype(jnp.float32)
    high[:, where] = (chosen >> 5).astype(jnp.float32)
    split_column = meta[:classes, features + 1 : features + 2]
    left[:, where] = (picked[pairs:] <= split_column).astype(jnp.float32)

    @pl.when(step == last)
    def _():
        for k in range(1, n_cls):
            stat_copy(k).wait()
        local_max = stats[0, 0:1, :]
        highest = local_max
        for k in range(1, n_cls):
            highest = jnp.maximum(highest, stats[k, 0:1, :])
        denom = stats[0, 1:2, :] * jnp.exp(local_max - highest)
        for k in range(1, n_cls):
            denom = denom + stats[k, 1:2, :] * jnp.exp(stats[k, 0:1, :] - highest)
        probs = jnp.exp(x_ref[...] - highest) / denom
        class_ids = cls * classes + lax.broadcasted_iota(jnp.int32, probs.shape, 0)
        target = (labels_ref[...] == class_ids).astype(jnp.float32)
        grad = (probs - target).astype(jnp.bfloat16).astype(jnp.float32)
        hess = (probs * (1.0 - probs)).astype(jnp.bfloat16).astype(jnp.float32)
        grad_ref[...] = grad
        hess_ref[...] = hess
        goes = left[...]
        lane = lax.broadcasted_iota(jnp.int32, (classes, 128), 1)
        total = jnp.where(lane == 0, jnp.sum(grad * goes, axis=1, keepdims=True), 0.0)
        total = jnp.where(lane == 1, jnp.sum(hess * goes, axis=1, keepdims=True), total)
        total = jnp.where(lane == 2, jnp.sum(grad, axis=1, keepdims=True), total)
        total = jnp.where(lane == 3, jnp.sum(hess, axis=1, keepdims=True), total)
        sums[0] = total
        for k in range(1, n_row):
            sum_copy(k).start()

        is_grad = lax.broadcasted_iota(jnp.int32, (2 * HIGH, rows), 0) < HIGH

        def expand(c, carry):
            mixed = jnp.where(is_grad, grad_ref[pl.ds(c, 1), :], hess_ref[pl.ds(c, 1), :])
            weights[pl.ds(pl.multiple_of(c * 2 * HIGH, 2 * HIGH), 2 * HIGH), :] = mixed.astype(
                jnp.bfloat16
            )
            return carry

        lax.fori_loop(0, classes, expand, 0)

        sub = lax.broadcasted_iota(jnp.int32, (16, chunk), 0)
        low_first = sub.astype(jnp.float32).astype(jnp.bfloat16)
        low_second = (sub + 16).astype(jnp.float32).astype(jnp.bfloat16)
        high_ids = (sub & (HIGH - 1)).astype(jnp.float32).astype(jnp.bfloat16)
        one = jnp.ones((16, chunk), jnp.bfloat16)
        zero = jnp.zeros((16, chunk), jnp.bfloat16)
        lane_pair = lax.broadcasted_iota(jnp.int32, (2 * HIGH, group * LOW), 1) // LOW

        def one_group(g):
            total = None
            for part in range(rows // chunk):
                cols = pl.ds(part * chunk, chunk)
                lows = []
                highs = []
                for j in range(group):
                    q = g * group + j
                    c = q // features
                    p = (q - c * features) * classes + c
                    lo = jnp.broadcast_to(low[pl.ds(p, 1), cols], (16, chunk)).astype(jnp.bfloat16)
                    hi = jnp.broadcast_to(high[pl.ds(p, 1), cols], (16, chunk)).astype(jnp.bfloat16)
                    w = weights[pl.ds(pl.multiple_of(c * 16, 16), 16), cols]
                    lows.append(jnp.where(lo == low_first, one, zero))
                    lows.append(jnp.where(lo == low_second, one, zero))
                    highs.append(jnp.where(hi == high_ids, w, zero))
                product = lax.dot_general(
                    jnp.concatenate(highs, axis=0), jnp.concatenate(lows, axis=0), NT,
                    preferred_element_type=jnp.float32,
                )
                total = product if total is None else total + product
            kept = total[:16]
            for j in range(1, group):
                kept = jnp.where(lane_pair == j, total[16 * j : 16 * j + 16], kept)
            return kept

        def fill(target_ref, s, dest):
            def some(i, carry):
                for u in range(unroll):
                    target_ref[s, i * unroll + u] = one_group(dest * groups_each + i * unroll + u)
                return carry

            lax.fori_loop(0, groups_each // unroll, some, 0)

        def pass_on(s):
            one_copy(s).wait_recv()
            mine[s] = mine[s] + first[s]
            two_copy(s).start()

        def each_chip(s, carry):
            dest = lax.rem(chip + s + 1, chips)
            fill(theirs, s, 2 * dest + 1 - core)
            one_copy(s).start()
            fill(mine, s, 2 * dest + core)

            @pl.when(s < chips - 1)
            def _():
                pass_on(s)

            return carry

        lax.fori_loop(0, chips, each_chip, 0)

        total = sums[0]
        for k in range(1, n_row):
            sum_copy(k).wait()
            total = total + sums[k]
        grad_left = total[:, 0:1]
        hess_left = total[:, 1:2]
        left_leaf = -grad_left / (hess_left + reg_lambda)
        right_leaf = -(total[:, 2:3] - grad_left) / (total[:, 3:4] - hess_left + reg_lambda)
        new_ref[...] = x_ref[...] + step_rate * jnp.where(left[...] > 0.5, left_leaf, right_leaf)

        one_copy(chips - 1).wait_recv()
        summed = mine[chips - 1] + first[chips - 1]
        for s in range(chips):
            one_copy(s).wait_send()
        for s in range(chips - 1):
            two_copy(s).wait()
            summed = summed + second[s]
        wide = group * LOW
        here = summed.reshape(groups_each * 2 * HIGH, wide)
        a = lax.broadcasted_iota(jnp.int32, (wide, wide), 0)
        b = lax.broadcasted_iota(jnp.int32, (wide, wide), 1)
        same = (a // LOW) == (b // LOW)
        upto = (same & (a <= b)).astype(jnp.float32)
        every = same.astype(jnp.float32)
        inside = jnp.dot(here, upto, precision=lax.Precision.HIGHEST, preferred_element_type=jnp.float32)
        whole = jnp.dot(here, every, precision=lax.Precision.HIGHEST, preferred_element_type=jnp.float32)
        count = groups_each * 2 * HIGH
        r = lax.broadcasted_iota(jnp.int32, (count, count), 0)
        s = lax.broadcasted_iota(jnp.int32, (count, count), 1)
        same_high = (r // HIGH) == (s // HIGH)
        before = jnp.dot((same_high & (s < r)).astype(jnp.float32), whole,
                         precision=lax.Precision.HIGHEST, preferred_element_type=jnp.float32)
        ends = jnp.dot(same_high.astype(jnp.float32), whole,
                       precision=lax.Precision.HIGHEST, preferred_element_type=jnp.float32)
        running = inside + before
        for g in range(groups_each):
            top = g * 2 * HIGH
            gl = running[top : top + HIGH]
            hl = running[top + HIGH : top + 2 * HIGH]
            ga = ends[top : top + HIGH]
            ha = ends[top + HIGH : top + 2 * HIGH]
            gains_ref[g] = (
                gl * gl / (hl + reg_lambda)
                + (ga - gl) * (ga - gl) / (ha - hl + reg_lambda)
                - ga * ga / (ha + reg_lambda)
            )


def local(n_cls, n_row, binned, labels, logits, elected, split_slot, split_bin):
    rows, classes = logits.shape
    columns = binned.shape[1]
    features = elected.shape[1]
    pairs = classes * features
    share = classes // n_row
    group = math.gcd(share * features, 8)
    groups_each = share * features // group
    block = math.gcd(rows, BLOCK)
    chunk = math.gcd(rows, CHUNK)
    unroll = math.gcd(groups_each, UNROLL)
    chips = n_row // 2
    f32 = jnp.float32
    dma = pltpu.SemaphoreType.DMA
    part = (chips, groups_each, 2 * HIGH, group * LOW)

    def whole(*shape):
        return pl.BlockSpec(shape, lambda i: (0,) * len(shape))

    new, gains = pl.pallas_call(
        functools.partial(kernel, n_cls, n_row, group, groups_each, chunk, unroll),
        grid=(rows // block,),
        out_shape=[
            jax.ShapeDtypeStruct((classes, rows), f32),
            jax.ShapeDtypeStruct((groups_each, HIGH, group * LOW), f32),
        ],
        in_specs=[
            pl.BlockSpec((block, columns), lambda i: (i, 0)),
            whole(classes, rows),
            whole(1, rows),
            whole(features, classes),
            whole(1, classes),
            whole(1, classes),
        ],
        out_specs=[whole(classes, rows), whole(groups_each, HIGH, group * LOW)],
        scratch_shapes=[
            pltpu.VMEM((128, 128), f32),
            pltpu.VMEM((pairs + classes, columns), jnp.bfloat16),
            pltpu.VMEM((pairs, rows), f32),
            pltpu.VMEM((pairs, rows), f32),
            pltpu.VMEM((classes, rows), f32),
            pltpu.VMEM((classes * 2 * HIGH, rows), jnp.bfloat16),
            pltpu.VMEM((classes, rows), f32),
            pltpu.VMEM((classes, rows), f32),
            pltpu.VMEM((n_cls, 2, rows), f32),
            pltpu.VMEM((n_row, classes, 128), f32),
            pltpu.VMEM(part, f32), pltpu.VMEM(part, f32), pltpu.VMEM(part, f32), pltpu.VMEM(part, f32),
            dma((n_cls,)), dma((n_cls,)), dma((n_row,)), dma((n_row,)),
            dma((chips,)), dma((chips,)), dma((chips,)), dma((chips,)),
        ],
        compiler_params=pltpu.CompilerParams(
            dimension_semantics=("arbitrary",), vmem_limit_bytes=56 * 1024 * 1024,
            collective_id=0, has_side_effects=True,
        ),
        name="round",
    )(
        binned, logits.T, labels.reshape(1, rows), elected.T,
        split_slot.reshape(1, classes), split_bin.reshape(1, classes),
    )
    gains = gains.reshape(groups_each, HIGH, group, LOW).transpose(0, 2, 1, 3)
    new = with_layout_constraint(new.T, Layout((1, 0)))
    return new, gains.reshape(share, features, BINS)


def solution(mesh):
    return jax.shard_map(
        functools.partial(local, mesh.shape["cls"], mesh.shape["row"]),
        mesh=mesh,
        in_specs=(P("row", None), P("row"), P("row", "cls"), P("cls", None), P("cls"), P("cls")),
        out_specs=(P("row", "cls"), P(("cls", "row"), None, None)),
        check_vma=False,
    )
```
